32 devices in a mesh: sp: 8 (over z, y), tp: 4 (over x, core).
Axes of the slice: x: 2, y: 2, z: 4, core: 2. Of those that a mesh axis runs over, the one named last changes fastest.
Arguments:
- decay_rate: float32 [1, 4096, 4096], P(None, 'sp', 'tp'), may hold values from 0.2 to 2
- drive_in: bfloat16 [1, 4096, 4096], P(None, 'sp', 'tp'), may hold values from -6 to 6
- gate_in: bfloat16 [1, 4096, 4096], P(None, 'sp', 'tp'), may hold values from -6 to 6
- norm_gain: float32 [4096], P('tp'), may hold values from 0.25 to 1.75
Outputs:
- filtered: bfloat16 [1, 4096, 4096], P(None, 'sp', 'tp')
The draws below stay inside these ranges and needn't reach their ends.
All inputs are finite; a program needn't handle non-finite values.
Results may differ from the reference program's by a relative error of at most 0.001.
Values sent between devices are 32-bit elements; how exact they have to be, the bound alone decides.
No kernel may reach another device: no remote copies, remote signals or barrier semaphores. Data moves between devices by JAX's collectives and lax.ppermute only.
A program may use at most 64 MiB of HBM per device.

```python
import jax
import jax.numpy as jnp
from jax import lax

BATCH = 1
CHANNELS = 4096
LENGTH = 4096


def block_levels(key, extent, cuts, smallest, largest):
    def one(dim, shards_of):
        steps = jax.random.uniform(jax.random.fold_in(jax.random.fold_in(key, 6), dim), (shards_of,), jnp.float32, smallest / len(cuts), largest / len(cuts))
        return jnp.repeat(jnp.exp(steps), extent[dim] // shards_of).reshape((-1,) + (1,) * (len(extent) - dim - 1))

    loudness = one(*cuts[0])
    for cut in cuts[1:]:
        loudness = loudness * one(*cut)
    return loudness


def scatter_about(own_key, shape, width, reach, shards=(), held_as=jnp.bfloat16):
    entries = jax.random.normal(own_key, shape, jnp.float32) * width
    if len(shards) > 0:
        entries = block_levels(own_key, shape, shards, -0.22, 0.18) * entries
    return jnp.clip(entries, min=-reach, max=reach).astype(held_as)


def setup_inputs(seed: int = 0) -> dict:
    key_list = jax.random.split(jax.random.key(seed), 5)
    decay_rate = jnp.clip(0.2 + 1.8 * jax.random.uniform(key_list[0], (BATCH, LENGTH, CHANNELS), jnp.float32) ** block_levels(key_list[0], (BATCH, LENGTH, CHANNELS), ((1, 8), (2, 4)), -0.2, 0.2), 0.2, 2.0)
    drive_in = scatter_about(key_list[1], (BATCH, LENGTH, CHANNELS), 1.0, 6.0, ((1, 8), (2, 4)))
    gate_in = scatter_about(key_list[2], (BATCH, LENGTH, CHANNELS), 1.0, 6.0, ((1, 8), (2, 4)))
    norm_gain = jnp.clip(1.0 + 0.15 * jax.random.normal(key_list[3], (CHANNELS,), jnp.float32), 0.25, 1.75)
    return {"decay_rate": decay_rate, "drive_in": drive_in, "gate_in": gate_in, "norm_gain": norm_gain}


def join_pair(earlier, later):
    return (earlier[0] * later[0], later[0] * earlier[1] + later[1])

def reference(decay_rate, drive_in, gate_in, norm_gain):
    keep = jnp.exp(-decay_rate / LENGTH)
    push = drive_in.astype(jnp.float32) * LENGTH ** (-0.5)
    forward = lax.associative_scan(join_pair, (keep, push), axis=1)[1]
    backward = lax.associative_scan(join_pair, (keep, push), axis=1, reverse=True)[1]
    states = forward + backward
    gated = states * jax.nn.sigmoid(gate_in.astype(jnp.float32))
    power = lax.optimization_barrier(jnp.mean(gated * gated, axis=-1, keepdims=True))
    filtered = (gated * lax.rsqrt(power + 1e-06) * norm_gain).astype(jnp.bfloat16)
    return filtered
```

```python
import functools

import jax
import jax.numpy as jnp
from jax import lax
from jax.experimental import pallas as pl
from jax.experimental.pallas import tpu as pltpu
from jax.sharding import PartitionSpec as P

LANES = 128
SEGMENTS = 8


def totals_kernel(scale, root, decay_ref, drive_ref, own_ref, prod_ref, first_ref, last_ref, rate_ref, push_ref):
    rows, width = decay_ref.shape
    steps = rows // SEGMENTS
    tiles = width // LANES

    def spread(m, _):
        for s in range(SEGMENTS):
            src = pl.ds(pl.multiple_of(s * steps + m * 16, 16), 16)
            for j in range(tiles):
                lanes = pl.ds(j * LANES, LANES)
                decay = decay_ref[src, lanes] * scale
                push = drive_ref[src, lanes].astype(jnp.float32) * root
                for h in range(2):
                    dst = pl.ds(j * rows + m * 16 * SEGMENTS + h * 8 * SEGMENTS + s, 8, stride=SEGMENTS)
                    rate_ref[dst, :] = decay[h * 8 : h * 8 + 8]
                    push_ref[dst, :] = push[h * 8 : h * 8 + 8]
        return 0

    lax.fori_loop(0, steps // 16, spread, 0)

    def step(i, carry):
        out = []
        for j in range(tiles):
            prod, fwd, bwd = carry[j]
            at = pl.ds(pl.multiple_of(j * rows + i * SEGMENTS, SEGMENTS), SEGMENTS)
            keep = jnp.exp(-rate_ref[at, :])
            push = push_ref[at, :]
            bwd = bwd + prod * push
            fwd = keep * fwd + push
            prod = prod * keep
            out.append((prod, fwd, bwd))
        return tuple(out)

    one = jnp.ones((SEGMENTS, LANES), jnp.float32)
    zero = jnp.zeros((SEGMENTS, LANES), jnp.float32)
    carry = lax.fori_loop(0, steps, step, ((one, zero, zero),) * tiles, unroll=8)
    for j in range(tiles):
        lanes = pl.ds(j * LANES, LANES)
        prod, fwd, bwd = carry[j]
        prod_ref[:, lanes] = prod
        first_ref[:, lanes] = fwd
        last_ref[:, lanes] = bwd
        p, f, b = prod[0:1], fwd[0:1], bwd[0:1]
        for s in range(1, SEGMENTS):
            b = b + p * bwd[s : s + 1]
            f = prod[s : s + 1] * f + fwd[s : s + 1]
            p = p * prod[s : s + 1]
        own_ref[0:1, lanes] = p
        own_ref[1:2, lanes] = f
        own_ref[2:3, lanes] = b
        own_ref[3:4, lanes] = jnp.zeros_like(b)


def states_kernel(mine_ref, all_ref, prod_ref, first_ref, last_ref, rate_ref, push_ref, gate_ref, gated_ref, power_ref, ent_ref, acc_ref, state_ref):
    rows, width = gate_ref.shape
    steps = rows // SEGMENTS
    tiles = width // LANES
    count = all_ref.shape[0]
    mine = mine_ref[0]
    fwd = jnp.zeros((1, width), jnp.float32)
    bwd = jnp.zeros((1, width), jnp.float32)
    for n in range(count):
        fwd = jnp.where(n < mine, all_ref[n, 0:1, :] * fwd + all_ref[n, 1:2, :], fwd)
    for n in range(count - 1, -1, -1):
        bwd = jnp.where(n > mine, all_ref[n, 0:1, :] * bwd + all_ref[n, 2:3, :], bwd)
    for s in range(SEGMENTS):
        ent_ref[0, s : s + 1, :] = fwd
        fwd = prod_ref[s : s + 1, :] * fwd + first_ref[s : s + 1, :]
    for s in range(SEGMENTS - 1, -1, -1):
        bwd = prod_ref[s : s + 1, :] * bwd + last_ref[s : s + 1, :]
        ent_ref[1, s : s + 1, :] = bwd

    group = 4 if tiles % 4 == 0 else 1
    for g in range(0, tiles, group):

        def step(i, carry):
            out = []
            for j in range(group):
                f, b = carry[j]
                at = pl.ds(pl.multiple_of((g + j) * rows + i * SEGMENTS, SEGMENTS), SEGMENTS)
                x = rate_ref[at, :]
                push = push_ref[at, :]
                f = jnp.exp(-x) * f + push
                state_ref[at, :] = f + b
                b = (b - push) * jnp.exp(x)
                out.append((f, b))
            return tuple(out)

        start = tuple(
            (ent_ref[0, :, pl.ds((g + j) * LANES, LANES)], ent_ref[1, :, pl.ds((g + j) * LANES, LANES)])
            for j in range(group)
        )
        lax.fori_loop(0, steps, step, start, unroll=8)

    def gating(m, _):
        for s in range(SEGMENTS):
            at = pl.ds(pl.multiple_of(s * steps + m * 16, 16), 16)
            acc = jnp.zeros((16, LANES), jnp.float32)
            for j in range(tiles):
                lanes = pl.ds(j * LANES, LANES)
                base = j * rows + m * 16 * SEGMENTS + s
                half = [state_ref[pl.ds(base + h * 8 * SEGMENTS, 8, stride=SEGMENTS), :] for h in range(2)]
                g = jnp.concatenate(half, axis=0) / (1.0 + jnp.exp(-gate_ref[at, lanes].astype(jnp.float32)))
                gated_ref[at, lanes] = g
                acc = acc + g * g
            acc_ref[at, :] = acc
        return 0

    lax.fori_loop(0, steps // 16, gating, 0)
    for r in range(rows // LANES):
        block = acc_ref[r * LANES : (r + 1) * LANES, :].T
        power_ref[r : r + 1, :] = jnp.sum(block, axis=0, keepdims=True)


def norm_kernel(channels, power_ref, gain_ref, gated_ref, out_ref):
    rows, width = gated_ref.shape
    for r in range(rows // LANES):
        total = power_ref[0, pl.ds(r, 1), :]
        for n in range(1, power_ref.shape[0]):
            total = total + power_ref[n, pl.ds(r, 1), :]
        factor = lax.rsqrt(total / channels + 1e-06)
        factor = jnp.broadcast_to(factor, (LANES, LANES)).T
        at = slice(r * LANES, (r + 1) * LANES)
        for j in range(width // LANES):
            lanes = slice(j * LANES, (j + 1) * LANES)
            out_ref[at, lanes] = (gated_ref[at, lanes] * factor * gain_ref[:, lanes]).astype(jnp.bfloat16)


def body(decay_rate, drive_in, gate_in, norm_gain):
    batch, rows, width = decay_rate.shape
    length = rows * lax.axis_size("sp")
    channels = width * lax.axis_size("tp")
    f32 = jnp.float32
    decay = decay_rate.reshape(rows, width)
    drive = drive_in.reshape(rows, width)
    gate = gate_in.reshape(rows, width)
    block = min(width, 256)
    vmem = pl.BlockSpec(memory_space=pltpu.VMEM)
    cols = lambda r: pl.BlockSpec((r, block), lambda c: (0, c))
    stack = pl.BlockSpec((rows * block // LANES, LANES), lambda c: (c, 0))
    own, prod, first, last, rate, push = pl.pallas_call(
        functools.partial(totals_kernel, 1.0 / length, length ** (-0.5)),
        grid=(width // block,),
        in_specs=[cols(rows), cols(rows)],
        out_specs=[cols(4), cols(SEGMENTS), cols(SEGMENTS), cols(SEGMENTS), stack, stack],
        out_shape=[jax.ShapeDtypeStruct((4, width), f32)]
        + [jax.ShapeDtypeStruct((SEGMENTS, width), f32)] * 3
        + [jax.ShapeDtypeStruct((rows * width // LANES, LANES), f32)] * 2,
        name="totals",
    )(decay, drive)
    everyone = lax.all_gather(own, "sp")
    mine = lax.axis_index("sp").astype(jnp.int32).reshape(1)
    gated, power = pl.pallas_call(
        states_kernel,
        in_specs=[pl.BlockSpec(memory_space=pltpu.SMEM)] + [vmem] * 7,
        out_specs=[vmem, vmem],
        out_shape=[jax.ShapeDtypeStruct((rows, width), f32), jax.ShapeDtypeStruct((rows // LANES, LANES), f32)],
        scratch_shapes=[pltpu.VMEM((2, SEGMENTS, width), f32), pltpu.VMEM((rows, LANES), f32), pltpu.VMEM((rows * width // LANES, LANES), f32)],
        name="states",
    )(mine, everyone, prod, first, last, rate, push, gate)
    powers = lax.all_gather(power, "tp")
    filtered = pl.pallas_call(
        functools.partial(norm_kernel, float(channels)),
        in_specs=[vmem, vmem, vmem],
        out_specs=vmem,
        out_shape=jax.ShapeDtypeStruct((rows, width), jnp.bfloat16),
        name="norm",
    )(powers, norm_gain.reshape(1, width), gated)
    return filtered.reshape(batch, rows, width)


def solution(mesh):
    in_specs = (P(None, "sp", "tp"), P(None, "sp", "tp"), P(None, "sp", "tp"), P("tp"))
    out_specs = P(None, "sp", "tp")
    return jax.shard_map(body, mesh=mesh, in_specs=in_specs, out_specs=out_specs, check_vma=False)
```

```python
import functools

import jax
import jax.numpy as jnp
from jax import lax
from jax.experimental import pallas as pl
from jax.experimental.pallas import tpu as pltpu
from jax.sharding import PartitionSpec as P

LANES = 128
SEGMENTS = 8


def totals_kernel(scale, root, decay_ref, drive_ref, own_ref, prod_ref, first_ref, last_ref, rate_ref, push_ref):
    rows, width = decay_ref.shape
    steps = rows // SEGMENTS
    tiles = width // LANES

    def spread(m, _):
        for s in range(SEGMENTS):
            src = pl.ds(pl.multiple_of(s * steps + m * 16, 16), 16)
            for j in range(tiles):
                lanes = pl.ds(j * LANES, LANES)
                decay = decay_ref[src, lanes] * scale
                push = drive_ref[src, lanes].astype(jnp.float32) * root
                for h in range(2):
                    dst = pl.ds(j * rows + m * 16 * SEGMENTS + h * 8 * SEGMENTS + s, 8, stride=SEGMENTS)
                    rate_ref[dst, :] = decay[h * 8 : h * 8 + 8]
                    push_ref[dst, :] = push[h * 8 : h * 8 + 8]
        return 0

    lax.fori_loop(0, steps // 16, spread, 0)

    def step(i, carry):
        out = []
        for j in range(tiles):
            prod, fwd, bwd = carry[j]
            at = pl.ds(pl.multiple_of(j * rows + i * SEGMENTS, SEGMENTS), SEGMENTS)
            keep = jnp.exp(-rate_ref[at, :])
            push = push_ref[at, :]
            bwd = bwd + prod * push
            fwd = keep * fwd + push
            prod = prod * keep
            out.append((prod, fwd, bwd))
        return tuple(out)

    one = jnp.ones((SEGMENTS, LANES), jnp.float32)
    zero = jnp.zeros((SEGMENTS, LANES), jnp.float32)
    carry = lax.fori_loop(0, steps, step, ((one, zero, zero),) * tiles, unroll=8)
    for j in range(tiles):
        lanes = pl.ds(j * LANES, LANES)
        prod, fwd, bwd = carry[j]
        prod_ref[:, lanes] = prod
        first_ref[:, lanes] = fwd
        last_ref[:, lanes] = bwd
        p, f, b = prod[0:1], fwd[0:1], bwd[0:1]
        for s in range(1, SEGMENTS):
            b = b + p * bwd[s : s + 1]
            f = prod[s : s + 1] * f + fwd[s : s + 1]
            p = p * prod[s : s + 1]
        own_ref[0:1, lanes] = p
        own_ref[1:2, lanes] = f
        own_ref[2:3, lanes] = b
        own_ref[3:4, lanes] = jnp.zeros_like(b)


def states_kernel(count, mine_ref, *refs):
    part_refs = refs[: count - 1]
    states_local(count, mine_ref, part_refs, *refs[count - 1 :])


def states_local(count, mine_ref, part_refs, prod_ref, first_ref, last_ref, rate_ref, push_ref, gate_ref, gated_ref, power_ref, ent_ref, acc_ref, state_ref):
    rows, width = gate_ref.shape
    steps = rows // SEGMENTS
    tiles = width // LANES
    mine = mine_ref[0]
    fwd = jnp.zeros((1, width), jnp.float32)
    bwd = jnp.zeros((1, width), jnp.float32)
    for k in range(count - 1, 0, -1):
        part = part_refs[k - 1]
        fwd = jnp.where(k <= mine, part[0:1, :] * fwd + part[1:2, :], fwd)
        part = part_refs[count - k - 1]
        bwd = jnp.where(mine + k < count, part[0:1, :] * bwd + part[2:3, :], bwd)
    for s in range(SEGMENTS):
        ent_ref[0, s : s + 1, :] = fwd
        fwd = prod_ref[s : s + 1, :] * fwd + first_ref[s : s + 1, :]
    for s in range(SEGMENTS - 1, -1, -1):
        bwd = prod_ref[s : s + 1, :] * bwd + last_ref[s : s + 1, :]
        ent_ref[1, s : s + 1, :] = bwd

    group = 4 if tiles % 4 == 0 else 1
    for g in range(0, tiles, group):

        def step(i, carry):
            out = []
            for j in range(group):
                f, b = carry[j]
                at = pl.ds(pl.multiple_of((g + j) * rows + i * SEGMENTS, SEGMENTS), SEGMENTS)
                x = rate_ref[at, :]
                push = push_ref[at, :]
                f = jnp.exp(-x) * f + push
                state_ref[at, :] = f + b
                b = (b - push) * jnp.exp(x)
                out.append((f, b))
            return tuple(out)

        start = tuple(
            (ent_ref[0, :, pl.ds((g + j) * LANES, LANES)], ent_ref[1, :, pl.ds((g + j) * LANES, LANES)])
            for j in range(group)
        )
        lax.fori_loop(0, steps, step, start, unroll=8)

    def gating(m, _):
        for s in range(SEGMENTS):
            at = pl.ds(pl.multiple_of(s * steps + m * 16, 16), 16)
            acc = jnp.zeros((16, LANES), jnp.float32)
            for j in range(tiles):
                lanes = pl.ds(j * LANES, LANES)
                base = j * rows + m * 16 * SEGMENTS + s
                half = [state_ref[pl.ds(base + h * 8 * SEGMENTS, 8, stride=SEGMENTS), :] for h in range(2)]
                g = jnp.concatenate(half, axis=0) / (1.0 + jnp.exp(-gate_ref[at, lanes].astype(jnp.float32)))
                gated_ref[at, lanes] = g
                acc = acc + g * g
            acc_ref[at, :] = acc
        return 0

    lax.fori_loop(0, steps // 16, gating, 0)
    for r in range(rows // LANES):
        block = acc_ref[r * LANES : (r + 1) * LANES, :].T
        power_ref[r : r + 1, :] = jnp.sum(block, axis=0, keepdims=True)


def norm_kernel(channels, *refs):
    *power_refs, gain_ref, gated_ref, out_ref = refs
    rows, width = gated_ref.shape
    for r in range(rows // LANES):
        total = power_refs[0][r : r + 1, :]
        for power_ref in power_refs[1:]:
            total = total + power_ref[r : r + 1, :]
        factor = lax.rsqrt(total / channels + 1e-06)
        factor = jnp.broadcast_to(factor, (LANES, LANES)).T
        at = slice(r * LANES, (r + 1) * LANES)
        for j in range(width // LANES):
            lanes = slice(j * LANES, (j + 1) * LANES)
            out_ref[at, lanes] = (gated_ref[at, lanes] * factor * gain_ref[:, lanes]).astype(jnp.bfloat16)


def shifts(value, axis):
    count = lax.axis_size(axis)
    return [
        lax.ppermute(value, axis, [(n, (n + k) % count) for n in range(count)])
        for k in range(1, count)
    ]


def body(decay_rate, drive_in, gate_in, norm_gain):
    batch, rows, width = decay_rate.shape
    length = rows * lax.axis_size("sp")
    channels = width * lax.axis_size("tp")
    f32 = jnp.float32
    decay = decay_rate.reshape(rows, width)
    drive = drive_in.reshape(rows, width)
    gate = gate_in.reshape(rows, width)
    block = min(width, 256)
    vmem = pl.BlockSpec(memory_space=pltpu.VMEM)
    cols = lambda r: pl.BlockSpec((r, block), lambda c: (0, c))
    stack = pl.BlockSpec((rows * block // LANES, LANES), lambda c: (c, 0))
    own, prod, first, last, rate, push = pl.pallas_call(
        functools.partial(totals_kernel, 1.0 / length, length ** (-0.5)),
        grid=(width // block,),
        in_specs=[cols(rows), cols(rows)],
        out_specs=[cols(4), cols(SEGMENTS), cols(SEGMENTS), cols(SEGMENTS), stack, stack],
        out_shape=[jax.ShapeDtypeStruct((4, width), f32)]
        + [jax.ShapeDtypeStruct((SEGMENTS, width), f32)] * 3
        + [jax.ShapeDtypeStruct((rows * width // LANES, LANES), f32)] * 2,
        name="totals",
    )(decay, drive)
    others = shifts(own, "sp")
    mine = lax.axis_index("sp").astype(jnp.int32).reshape(1)
    gated, power = pl.pallas_call(
        functools.partial(states_kernel, len(others) + 1),
        in_specs=[pl.BlockSpec(memory_space=pltpu.SMEM)] + [vmem] * (len(others) + 6),
        out_specs=[vmem, vmem],
        out_shape=[jax.ShapeDtypeStruct((rows, width), f32), jax.ShapeDtypeStruct((rows // LANES, LANES), f32)],
        scratch_shapes=[pltpu.VMEM((2, SEGMENTS, width), f32), pltpu.VMEM((rows, LANES), f32), pltpu.VMEM((rows * width // LANES, LANES), f32)],
        name="states",
    )(mine, *others, prod, first, last, rate, push, gate)
    powers = [power] + shifts(power, "tp")
    filtered = pl.pallas_call(
        functools.partial(norm_kernel, float(channels)),
        in_specs=[vmem] * (len(powers) + 2),
        out_specs=vmem,
        out_shape=jax.ShapeDtypeStruct((rows, width), jnp.bfloat16),
        name="norm",
    )(*powers, norm_gain.reshape(1, width), gated)
    return filtered.reshape(batch, rows, width)


def solution(mesh):
    in_specs = (P(None, "sp", "tp"), P(None, "sp", "tp"), P(None, "sp", "tp"), P("tp"))
    out_specs = P(None, "sp", "tp")
    return jax.shard_map(body, mesh=mesh, in_specs=in_specs, out_specs=out_specs, check_vma=False)
```

```python
import functools

import jax
import jax.numpy as jnp
from jax import lax
from jax.experimental import pallas as pl
from jax.experimental.pallas import tpu as pltpu
from jax.sharding import PartitionSpec as P

LANES = 128
SEGMENTS = 8


def totals_kernel(scale, root, decay_ref, drive_ref, own_ref, prod_ref, first_ref, last_ref, rate_ref, push_ref):
    rows, width = decay_ref.shape
    steps = rows // SEGMENTS
    tiles = width // LANES

    def spread(m, _):
        for s in range(SEGMENTS):
            src = pl.ds(pl.multiple_of(s * steps + m * 16, 16), 16)
            for j in range(tiles):
                lanes = pl.ds(j * LANES, LANES)
                decay = decay_ref[src, lanes] * scale
                push = drive_ref[src, lanes].astype(jnp.float32) * root
                for h in range(2):
                    dst = pl.ds(j * rows + m * 16 * SEGMENTS + h * 8 * SEGMENTS + s, 8, stride=SEGMENTS)
                    rate_ref[dst, :] = decay[h * 8 : h * 8 + 8]
                    push_ref[dst, :] = push[h * 8 : h * 8 + 8]
        return 0

    lax.fori_loop(0, steps // 16, spread, 0)

    def step(i, carry):
        out = []
        for j in range(tiles):
            prod, fwd, bwd = carry[j]
            at = pl.ds(pl.multiple_of(j * rows + i * SEGMENTS, SEGMENTS), SEGMENTS)
            keep = jnp.exp(-rate_ref[at, :])
            push = push_ref[at, :]
            bwd = bwd + prod * push
            fwd = keep * fwd + push
            prod = prod * keep
            out.append((prod, fwd, bwd))
        return tuple(out)

    one = jnp.ones((SEGMENTS, LANES), jnp.float32)
    zero = jnp.zeros((SEGMENTS, LANES), jnp.float32)
    carry = lax.fori_loop(0, steps, step, ((one, zero, zero),) * tiles, unroll=8)
    for j in range(tiles):
        lanes = pl.ds(j * LANES, LANES)
        prod, fwd, bwd = carry[j]
        prod_ref[:, lanes] = prod
        first_ref[:, lanes] = fwd
        last_ref[:, lanes] = bwd
        p, f, b = prod[0:1], fwd[0:1], bwd[0:1]
        for s in range(1, SEGMENTS):
            b = b + p * bwd[s : s + 1]
            f = prod[s : s + 1] * f + fwd[s : s + 1]
            p = p * prod[s : s + 1]
        for n in range(own_ref.shape[0]):
            own_ref[n, 0:1, lanes] = p
            own_ref[n, 1:2, lanes] = f
            own_ref[n, 2:3, lanes] = b
            own_ref[n, 3:4, lanes] = jnp.zeros_like(b)


def states_kernel(mine_ref, all_ref, prod_ref, first_ref, last_ref, rate_ref, push_ref, gate_ref, gated_ref, power_ref, ent_ref, acc_ref, state_ref):
    rows, width = gate_ref.shape
    steps = rows // SEGMENTS
    tiles = width // LANES
    count = all_ref.shape[0]
    mine = mine_ref[0]
    fwd = jnp.zeros((1, width), jnp.float32)
    bwd = jnp.zeros((1, width), jnp.float32)
    for n in range(count):
        fwd = jnp.where(n < mine, all_ref[n, 0:1, :] * fwd + all_ref[n, 1:2, :], fwd)
    for n in range(count - 1, -1, -1):
        bwd = jnp.where(n > mine, all_ref[n, 0:1, :] * bwd + all_ref[n, 2:3, :], bwd)
    for s in range(SEGMENTS):
        ent_ref[0, s : s + 1, :] = fwd
        fwd = prod_ref[s : s + 1, :] * fwd + first_ref[s : s + 1, :]
    for s in range(SEGMENTS - 1, -1, -1):
        bwd = prod_ref[s : s + 1, :] * bwd + last_ref[s : s + 1, :]
        ent_ref[1, s : s + 1, :] = bwd

    group = 4 if tiles % 4 == 0 else 1
    for g in range(0, tiles, group):

        def step(i, carry):
            out = []
            for j in range(group):
                f, b = carry[j]
                at = pl.ds(pl.multiple_of((g + j) * rows + i * SEGMENTS, SEGMENTS), SEGMENTS)
                x = rate_ref[at, :]
                push = push_ref[at, :]
                f = jnp.exp(-x) * f + push
                state_ref[at, :] = f + b
                b = (b - push) * jnp.exp(x)
                out.append((f, b))
            return tuple(out)

        start = tuple(
            (ent_ref[0, :, pl.ds((g + j) * LANES, LANES)], ent_ref[1, :, pl.ds((g + j) * LANES, LANES)])
            for j in range(group)
        )
        lax.fori_loop(0, steps, step, start, unroll=8)

    def gating(m, _):
        for s in range(SEGMENTS):
            at = pl.ds(pl.multiple_of(s * steps + m * 16, 16), 16)
            acc = jnp.zeros((16, LANES), jnp.float32)
            for j in range(tiles):
                lanes = pl.ds(j * LANES, LANES)
                base = j * rows + m * 16 * SEGMENTS + s
                half = [state_ref[pl.ds(base + h * 8 * SEGMENTS, 8, stride=SEGMENTS), :] for h in range(2)]
                g = jnp.concatenate(half, axis=0) / (1.0 + jnp.exp(-gate_ref[at, lanes].astype(jnp.float32)))
                gated_ref[at, lanes] = g
                acc = acc + g * g
            acc_ref[at, :] = acc
        return 0

    lax.fori_loop(0, steps // 16, gating, 0)
    for r in range(rows // LANES):
        block = acc_ref[r * LANES : (r + 1) * LANES, :].T
        power = jnp.sum(block, axis=0, keepdims=True)
        for n in range(power_ref.shape[0]):
            power_ref[n, r : r + 1, :] = power


def norm_kernel(channels, power_ref, gain_ref, gated_ref, out_ref):
    rows, width = gated_ref.shape
    for r in range(rows // LANES):
        total = power_ref[0, r : r + 1, :]
        for n in range(1, power_ref.shape[0]):
            total = total + power_ref[n, r : r + 1, :]
        factor = lax.rsqrt(total / channels + 1e-06)
        factor = jnp.broadcast_to(factor, (LANES, LANES)).T
        at = slice(r * LANES, (r + 1) * LANES)
        for j in range(width // LANES):
            lanes = slice(j * LANES, (j + 1) * LANES)
            out_ref[at, lanes] = (gated_ref[at, lanes] * factor * gain_ref[:, lanes]).astype(jnp.bfloat16)


def held(value):
    return pltpu.with_memory_space_constraint(value, pltpu.VMEM)


def body(decay_rate, drive_in, gate_in, norm_gain):
    batch, rows, width = decay_rate.shape
    length = rows * lax.axis_size("sp")
    channels = width * lax.axis_size("tp")
    f32 = jnp.float32
    decay = decay_rate.reshape(rows, width)
    drive = drive_in.reshape(rows, width)
    gate = gate_in.reshape(rows, width)
    block = min(width, 256)
    vmem = pl.BlockSpec(memory_space=pltpu.VMEM)
    cols = lambda r: pl.BlockSpec((r, block), lambda c: (0, c))
    stack = pl.BlockSpec((rows * block // LANES, LANES), lambda c: (c, 0))
    own, prod, first, last, rate, push = pl.pallas_call(
        functools.partial(totals_kernel, 1.0 / length, length ** (-0.5)),
        grid=(width // block,),
        in_specs=[cols(rows), cols(rows)],
        out_specs=[pl.BlockSpec((lax.axis_size("sp"), 4, block), lambda c: (0, 0, c)), cols(SEGMENTS), cols(SEGMENTS), cols(SEGMENTS), stack, stack],
        out_shape=[pltpu.VMEM((lax.axis_size("sp"), 4, width), f32)]
        + [pltpu.VMEM((SEGMENTS, width), f32)] * 3
        + [jax.ShapeDtypeStruct((rows * width // LANES, LANES), f32)] * 2,
        name="totals",
    )(decay, drive)
    others = held(lax.all_to_all(own, "sp", 0, 0, tiled=True))
    mine = lax.axis_index("sp").astype(jnp.int32).reshape(1)
    gated, power = pl.pallas_call(
        states_kernel,
        in_specs=[pl.BlockSpec(memory_space=pltpu.SMEM)] + [vmem] * 7,
        out_specs=[vmem, vmem],
        out_shape=[pltpu.VMEM((rows, width), f32), pltpu.VMEM((lax.axis_size("tp"), rows // LANES, LANES), f32)],
        scratch_shapes=[pltpu.VMEM((2, SEGMENTS, width), f32), pltpu.VMEM((rows, LANES), f32), pltpu.VMEM((rows * width // LANES, LANES), f32)],
        name="states",
    )(mine, others, held(prod), held(first), held(last), rate, push, gate)
    powers = held(lax.all_to_all(power, "tp", 0, 0, tiled=True))
    filtered = pl.pallas_call(
        functools.partial(norm_kernel, float(channels)),
        in_specs=[vmem] * 3,
        out_specs=vmem,
        out_shape=jax.ShapeDtypeStruct((rows, width), jnp.bfloat16),
        name="norm",
    )(powers, norm_gain.reshape(1, width), held(gated))
    return filtered.reshape(batch, rows, width)


def solution(mesh):
    in_specs = (P(None, "sp", "tp"), P(None, "sp", "tp"), P(None, "sp", "tp"), P("tp"))
    out_specs = P(None, "sp", "tp")
    return jax.shard_map(body, mesh=mesh, in_specs=in_specs, out_specs=out_specs, check_vma=False)
```

```python
import functools

import jax
import jax.numpy as jnp
from jax import lax
from jax.experimental import pallas as pl
from jax.experimental.pallas import tpu as pltpu
from jax.sharding import PartitionSpec as P

LANES = 128
SEGMENTS = 8


def spread(scale, root, decay_ref, drive_ref, rate_ref, push_ref):
    rows, width = decay_ref.shape
    steps = rows // SEGMENTS

    def some(m, _):
        for s in range(SEGMENTS):
            src = pl.ds(pl.multiple_of(s * steps + m * 16, 16), 16)
            for j in range(width // LANES):
                lanes = pl.ds(j * LANES, LANES)
                decay = decay_ref[src, lanes] * scale
                push = drive_ref[src, lanes].astype(jnp.float32) * root
                for h in range(2):
                    dst = pl.ds(j * rows + m * 16 * SEGMENTS + h * 8 * SEGMENTS + s, 8, stride=SEGMENTS)
                    rate_ref[dst, :] = decay[h * 8 : h * 8 + 8]
                    push_ref[dst, :] = push[h * 8 : h * 8 + 8]
        return 0

    lax.fori_loop(0, steps // 16, some, 0)


def totals_kernel(scale, root, decay_ref, drive_ref, own_ref, prod_ref, first_ref, last_ref, rate_ref, push_ref):
    rows, width = decay_ref.shape
    steps = rows // SEGMENTS
    tiles = width // LANES
    spread(scale, root, decay_ref, drive_ref, rate_ref, push_ref)

    def step(i, carry):
        out = []
        for j in range(tiles):
            prod, fwd, bwd = carry[j]
            at = pl.ds(pl.multiple_of(j * rows + i * SEGMENTS, SEGMENTS), SEGMENTS)
            keep = jnp.exp(-rate_ref[at, :])
            push = push_ref[at, :]
            bwd = bwd + prod * push
            fwd = keep * fwd + push
            prod = prod * keep
            out.append((prod, fwd, bwd))
        return tuple(out)

    one = jnp.ones((SEGMENTS, LANES), jnp.float32)
    zero = jnp.zeros((SEGMENTS, LANES), jnp.float32)
    carry = lax.fori_loop(0, steps, step, ((one, zero, zero),) * tiles, unroll=8)
    for j in range(tiles):
        lanes = pl.ds(j * LANES, LANES)
        prod, fwd, bwd = carry[j]
        prod_ref[:, lanes] = prod
        first_ref[:, lanes] = fwd
        last_ref[:, lanes] = bwd
        p, f, b = prod[0:1], fwd[0:1], bwd[0:1]
        for s in range(1, SEGMENTS):
            b = b + p * bwd[s : s + 1]
            f = prod[s : s + 1] * f + fwd[s : s + 1]
            p = p * prod[s : s + 1]
        for n in range(own_ref.shape[0]):
            own_ref[n, 0:1, lanes] = p
            own_ref[n, 1:2, lanes] = f
            own_ref[n, 2:3, lanes] = b
            own_ref[n, 3:4, lanes] = jnp.zeros_like(b)


def states_kernel(scale, root, mine_ref, all_ref, prod_ref, first_ref, last_ref, decay_ref, drive_ref, gate_ref, gated_ref, power_ref, ent_ref, acc_ref, state_ref, rate_ref, push_ref):
    spread(scale, root, decay_ref, drive_ref, rate_ref, push_ref)

    @pl.when(pl.program_id(0) == 0)
    def _():
        acc_ref[...] = jnp.zeros_like(acc_ref)

    rows, width = gate_ref.shape
    steps = rows // SEGMENTS
    tiles = width // LANES
    count = all_ref.shape[0]
    mine = mine_ref[0]
    fwd = jnp.zeros((1, width), jnp.float32)
    bwd = jnp.zeros((1, width), jnp.float32)
    for n in range(count):
        fwd = jnp.where(n < mine, all_ref[n, 0:1, :] * fwd + all_ref[n, 1:2, :], fwd)
    for n in range(count - 1, -1, -1):
        bwd = jnp.where(n > mine, all_ref[n, 0:1, :] * bwd + all_ref[n, 2:3, :], bwd)
    for s in range(SEGMENTS):
        ent_ref[0, s : s + 1, :] = fwd
        fwd = prod_ref[s : s + 1, :] * fwd + first_ref[s : s + 1, :]
    for s in range(SEGMENTS - 1, -1, -1):
        bwd = prod_ref[s : s + 1, :] * bwd + last_ref[s : s + 1, :]
        ent_ref[1, s : s + 1, :] = bwd

    group = tiles
    for g in range(0, tiles, group):

        def step(i, carry):
            out = []
            for j in range(group):
                f, b = carry[j]
                at = pl.ds(pl.multiple_of((g + j) * rows + i * SEGMENTS, SEGMENTS), SEGMENTS)
                x = rate_ref[at, :]
                push = push_ref[at, :]
                f = jnp.exp(-x) * f + push
                state_ref[at, :] = f + b
                b = (b - push) * jnp.exp(x)
                out.append((f, b))
            return tuple(out)

        start = tuple(
            (ent_ref[0, :, pl.ds((g + j) * LANES, LANES)], ent_ref[1, :, pl.ds((g + j) * LANES, LANES)])
            for j in range(group)
        )
        lax.fori_loop(0, steps, step, start, unroll=8)

    def gating(m, _):
        for s in range(SEGMENTS):
            at = pl.ds(pl.multiple_of(s * steps + m * 16, 16), 16)
            acc = acc_ref[at, :]
            for j in range(tiles):
                lanes = pl.ds(j * LANES, LANES)
                base = j * rows + m * 16 * SEGMENTS + s
                half = [state_ref[pl.ds(base + h * 8 * SEGMENTS, 8, stride=SEGMENTS), :] for h in range(2)]
                g = jnp.concatenate(half, axis=0) / (1.0 + jnp.exp(-gate_ref[at, lanes].astype(jnp.float32)))
                gated_ref[at, lanes] = g
                acc = acc + g * g
            acc_ref[at, :] = acc
        return 0

    lax.fori_loop(0, steps // 16, gating, 0)
    @pl.when(pl.program_id(0) == pl.num_programs(0) - 1)
    def _():
        for r in range(rows // LANES):
            block = acc_ref[r * LANES : (r + 1) * LANES, :].T
            power = jnp.sum(block, axis=0, keepdims=True)
            for n in range(power_ref.shape[0]):
                power_ref[n, r : r + 1, :] = power


def norm_kernel(channels, power_ref, gain_ref, gated_ref, out_ref):
    r = pl.ds(pl.program_id(0), 1)
    total = power_ref[0, r, :]
    for n in range(1, power_ref.shape[0]):
        total = total + power_ref[n, r, :]
    factor = lax.rsqrt(total / channels + 1e-06)
    factor = jnp.broadcast_to(factor, (LANES, LANES)).T
    for j in range(gated_ref.shape[1] // LANES):
        lanes = slice(j * LANES, (j + 1) * LANES)
        out_ref[:, lanes] = (gated_ref[:, lanes] * factor * gain_ref[:, lanes]).astype(jnp.bfloat16)


def held(value):
    return pltpu.with_memory_space_constraint(value, pltpu.VMEM)


def body(decay_rate, drive_in, gate_in, norm_gain):
    batch, rows, width = decay_rate.shape
    length = rows * lax.axis_size("sp")
    channels = width * lax.axis_size("tp")
    f32 = jnp.float32
    decay = decay_rate.reshape(rows, width)
    drive = drive_in.reshape(rows, width)
    gate = gate_in.reshape(rows, width)
    block = min(width, 256)
    cols = lambda r: pl.BlockSpec((r, block), lambda c: (0, c))
    scale, root = 1.0 / length, length ** (-0.5)
    places, peers = lax.axis_size("sp"), lax.axis_size("tp")
    stack = pltpu.VMEM((rows * block // LANES, LANES), f32)
    whole = lambda shape: pl.BlockSpec(shape, lambda c: (0,) * len(shape))
    whose = pl.BlockSpec((places, 4, block), lambda c: (0, 0, c))
    own, prod, first, last = pl.pallas_call(
        functools.partial(totals_kernel, scale, root),
        grid=(width // block,),
        in_specs=[cols(rows), cols(rows)],
        out_specs=[whose, cols(SEGMENTS), cols(SEGMENTS), cols(SEGMENTS)],
        out_shape=[pltpu.VMEM((places, 4, width), f32)] + [pltpu.VMEM((SEGMENTS, width), f32)] * 3,
        scratch_shapes=[stack, stack],
        name="totals",
    )(decay, drive)
    others = held(lax.all_to_all(own, "sp", 0, 0, tiled=True))
    mine = lax.axis_index("sp").astype(jnp.int32).reshape(1)
    gated, power = pl.pallas_call(
        functools.partial(states_kernel, scale, root),
        grid=(width // block,),
        in_specs=[pl.BlockSpec(memory_space=pltpu.SMEM), whose]
        + [cols(SEGMENTS)] * 3
        + [cols(rows)] * 3,
        out_specs=[cols(rows), whole((peers, rows // LANES, LANES))],
        out_shape=[
            jax.ShapeDtypeStruct((rows, width), f32),
            pltpu.VMEM((peers, rows // LANES, LANES), f32),
        ],
        scratch_shapes=[
            pltpu.VMEM((2, SEGMENTS, block), f32),
            pltpu.VMEM((rows, LANES), f32),
            stack,
            stack,
            stack,
        ],
        name="states",
    )(mine, others, held(prod), held(first), held(last), decay, drive, gate)
    powers = held(lax.all_to_all(power, "tp", 0, 0, tiled=True))
    span = pl.BlockSpec((LANES, width), lambda r: (r, 0))
    filtered = pl.pallas_call(
        functools.partial(norm_kernel, float(channels)),
        grid=(rows // LANES,),
        in_specs=[whole((peers, rows // LANES, LANES)), whole((1, width)), span],
        out_specs=span,
        out_shape=jax.ShapeDtypeStruct((rows, width), jnp.bfloat16),
        name="norm",
    )(powers, norm_gain.reshape(1, width), gated)
    return filtered.reshape(batch, rows, width)


def solution(mesh):
    in_specs = (P(None, "sp", "tp"), P(None, "sp", "tp"), P(None, "sp", "tp"), P("tp"))
    out_specs = P(None, "sp", "tp")
    return jax.shard_map(body, mesh=mesh, in_specs=in_specs, out_specs=out_specs, check_vma=False)
```

```python
import functools

import jax
import jax.numpy as jnp
from jax import lax
from jax.experimental import pallas as pl
from jax.experimental.pallas import tpu as pltpu
from jax.sharding import PartitionSpec as P

LANES = 128
SEGMENTS = 8


def totals_kernel(scale, root, mine_ref, decay_ref, drive_ref, own_ref, prod_ref, first_ref, last_ref, rate_ref, push_ref):
    rows, width = decay_ref.shape
    steps = rows // SEGMENTS
    tiles = width // LANES

    def spread(m, _):
        for s in range(SEGMENTS):
            src = pl.ds(pl.multiple_of(s * steps + m * 16, 16), 16)
            for j in range(tiles):
                lanes = pl.ds(j * LANES, LANES)
                decay = decay_ref[src, lanes] * scale
                push = drive_ref[src, lanes].astype(jnp.float32) * root
                for h in range(2):
                    dst = pl.ds(j * rows + m * 16 * SEGMENTS + h * 8 * SEGMENTS + s, 8, stride=SEGMENTS)
                    rate_ref[dst, :] = decay[h * 8 : h * 8 + 8]
                    push_ref[dst, :] = push[h * 8 : h * 8 + 8]
        return 0

    lax.fori_loop(0, steps // 16, spread, 0)

    def step(i, carry):
        out = []
        for j in range(tiles):
            prod, fwd, bwd = carry[j]
            at = pl.ds(pl.multiple_of(j * rows + i * SEGMENTS, SEGMENTS), SEGMENTS)
            keep = jnp.exp(-rate_ref[at, :])
            push = push_ref[at, :]
            bwd = bwd + prod * push
            fwd = keep * fwd + push
            prod = prod * keep
            out.append((prod, fwd, bwd))
        return tuple(out)

    one = jnp.ones((SEGMENTS, LANES), jnp.float32)
    zero = jnp.zeros((SEGMENTS, LANES), jnp.float32)
    carry = lax.fori_loop(0, steps, step, ((one, zero, zero),) * tiles, unroll=8)
    for j in range(tiles):
        lanes = pl.ds(j * LANES, LANES)
        prod, fwd, bwd = carry[j]
        prod_ref[:, lanes] = prod
        first_ref[:, lanes] = fwd
        last_ref[:, lanes] = bwd
        p, f, b = prod[0:1], fwd[0:1], bwd[0:1]
        for s in range(1, SEGMENTS):
            b = b + p * bwd[s : s + 1]
            f = prod[s : s + 1] * f + fwd[s : s + 1]
            p = p * prod[s : s + 1]
        for n in range(own_ref.shape[0]):
            own_ref[n, 0:1, lanes] = p
            own_ref[n, 1:2, lanes] = jnp.where(n > mine_ref[0], f, b)


def states_kernel(mine_ref, all_ref, prod_ref, first_ref, last_ref, rate_ref, push_ref, gate_ref, gated_ref, power_ref, ent_ref, acc_ref, state_ref):
    rows, width = gate_ref.shape
    steps = rows // SEGMENTS
    tiles = width // LANES
    count = all_ref.shape[0]
    mine = mine_ref[0]
    fwd = jnp.zeros((1, width), jnp.float32)
    bwd = jnp.zeros((1, width), jnp.float32)
    for n in range(count):
        fwd = jnp.where(n < mine, all_ref[n, 0:1, :] * fwd + all_ref[n, 1:2, :], fwd)
    for n in range(count - 1, -1, -1):
        bwd = jnp.where(n > mine, all_ref[n, 0:1, :] * bwd + all_ref[n, 1:2, :], bwd)
    for s in range(SEGMENTS):
        ent_ref[0, s : s + 1, :] = fwd
        fwd = prod_ref[s : s + 1, :] * fwd + first_ref[s : s + 1, :]
    for s in range(SEGMENTS - 1, -1, -1):
        bwd = prod_ref[s : s + 1, :] * bwd + last_ref[s : s + 1, :]
        ent_ref[1, s : s + 1, :] = bwd

    group = 4 if tiles % 4 == 0 else 1
    for g in range(0, tiles, group):

        def step(i, carry):
            out = []
            for j in range(group):
                f, b = carry[j]
                at = pl.ds(pl.multiple_of((g + j) * rows + i * SEGMENTS, SEGMENTS), SEGMENTS)
                x = rate_ref[at, :]
                push = push_ref[at, :]
                f = jnp.exp(-x) * f + push
                state_ref[at, :] = f + b
                b = (b - push) * jnp.exp(x)
                out.append((f, b))
            return tuple(out)

        start = tuple(
            (ent_ref[0, :, pl.ds((g + j) * LANES, LANES)], ent_ref[1, :, pl.ds((g + j) * LANES, LANES)])
            for j in range(group)
        )
        lax.fori_loop(0, steps, step, start, unroll=8)

    def gating(m, _):
        for s in range(SEGMENTS):
            at = pl.ds(pl.multiple_of(s * steps + m * 16, 16), 16)
            acc = jnp.zeros((16, LANES), jnp.float32)
            for j in range(tiles):
                lanes = pl.ds(j * LANES, LANES)
                base = j * rows + m * 16 * SEGMENTS + s
                half = [state_ref[pl.ds(base + h * 8 * SEGMENTS, 8, stride=SEGMENTS), :] for h in range(2)]
                g = jnp.concatenate(half, axis=0) / (1.0 + jnp.exp(-gate_ref[at, lanes].astype(jnp.float32)))
                gated_ref[at, lanes] = g
                acc = acc + g * g
            acc_ref[at, :] = acc
        return 0

    lax.fori_loop(0, steps // 16, gating, 0)
    for r in range(rows // LANES):
        block = acc_ref[r * LANES : (r + 1) * LANES, :].T
        power = jnp.sum(block, axis=0, keepdims=True)
        power_ref[r : r + 1, :] = power


def norm_kernel(channels, *refs):
    *power_refs, gain_ref, gated_ref, out_ref = refs
    rows, width = gated_ref.shape
    for r in range(rows // LANES):
        total = power_refs[0][r : r + 1, :]
        for power_ref in power_refs[1:]:
            total = total + power_ref[r : r + 1, :]
        factor = lax.rsqrt(total / channels + 1e-06)
        factor = jnp.broadcast_to(factor, (LANES, LANES)).T
        at = slice(r * LANES, (r + 1) * LANES)
        for j in range(width // LANES):
            lanes = slice(j * LANES, (j + 1) * LANES)
            out_ref[at, lanes] = (gated_ref[at, lanes] * factor * gain_ref[:, lanes]).astype(jnp.bfloat16)


def held(value):
    return pltpu.with_memory_space_constraint(value, pltpu.VMEM)


def shifts(value, axis):
    count = lax.axis_size(axis)
    return [
        held(lax.ppermute(value, axis, [(n, (n + k) % count) for n in range(count)]))
        for k in range(1, count)
    ]


def body(decay_rate, drive_in, gate_in, norm_gain):
    batch, rows, width = decay_rate.shape
    length = rows * lax.axis_size("sp")
    channels = width * lax.axis_size("tp")
    f32 = jnp.float32
    decay = decay_rate.reshape(rows, width)
    drive = drive_in.reshape(rows, width)
    gate = gate_in.reshape(rows, width)
    block = min(width, 256)
    vmem = pl.BlockSpec(memory_space=pltpu.VMEM)
    cols = lambda r: pl.BlockSpec((r, block), lambda c: (0, c))
    stack = pl.BlockSpec((rows * block // LANES, LANES), lambda c: (c, 0))
    mine = lax.axis_index("sp").astype(jnp.int32).reshape(1)
    own, prod, first, last, rate, push = pl.pallas_call(
        functools.partial(totals_kernel, 1.0 / length, length ** (-0.5)),
        grid=(width // block,),
        in_specs=[pl.BlockSpec(memory_space=pltpu.SMEM), cols(rows), cols(rows)],
        out_specs=[pl.BlockSpec((lax.axis_size("sp"), 2, block), lambda c: (0, 0, c)), cols(SEGMENTS), cols(SEGMENTS), cols(SEGMENTS), stack, stack],
        out_shape=[pltpu.VMEM((lax.axis_size("sp"), 2, width), f32)]
        + [pltpu.VMEM((SEGMENTS, width), f32)] * 3
        + [jax.ShapeDtypeStruct((rows * width // LANES, LANES), f32)] * 2,
        name="totals",
    )(mine, decay, drive)
    others = held(lax.all_to_all(own, "sp", 0, 0, tiled=True))
    gated, power = pl.pallas_call(
        states_kernel,
        in_specs=[pl.BlockSpec(memory_space=pltpu.SMEM)] + [vmem] * 7,
        out_specs=[vmem, vmem],
        out_shape=[pltpu.VMEM((rows, width), f32), pltpu.VMEM((rows // LANES, LANES), f32)],
        scratch_shapes=[pltpu.VMEM((2, SEGMENTS, width), f32), pltpu.VMEM((rows, LANES), f32), pltpu.VMEM((rows * width // LANES, LANES), f32)],
        name="states",
    )(mine, others, held(prod), held(first), held(last), rate, push, gate)
    powers = [held(power)] + shifts(power, "tp")
    filtered = pl.pallas_call(
        functools.partial(norm_kernel, float(channels)),
        in_specs=[vmem] * (len(powers) + 2),
        out_specs=vmem,
        out_shape=jax.ShapeDtypeStruct((rows, width), jnp.bfloat16),
        name="norm",
    )(*powers, norm_gain.reshape(1, width), held(gated))
    return filtered.reshape(batch, rows, width)


def solution(mesh):
    in_specs = (P(None, "sp", "tp"), P(None, "sp", "tp"), P(None, "sp", "tp"), P("tp"))
    out_specs = P(None, "sp", "tp")
    return jax.shard_map(body, mesh=mesh, in_specs=in_specs, out_specs=out_specs, check_vma=False)
```

```python
import functools

import jax
import jax.numpy as jnp
from jax import lax
from jax.experimental import pallas as pl
from jax.experimental.pallas import tpu as pltpu
from jax.sharding import PartitionSpec as P

LANES = 128
SEGMENTS = 8


def totals_kernel(scale, root, mine_ref, decay_ref, drive_ref, own_ref, prod_ref, first_ref, last_ref, rate_ref, push_ref):
    rows, width = decay_ref.shape
    steps = rows // SEGMENTS
    tiles = width // LANES

    def spread(m, _):
        for s in range(SEGMENTS):
            src = pl.ds(pl.multiple_of(s * steps + m * 16, 16), 16)
            for j in range(tiles):
                lanes = pl.ds(j * LANES, LANES)
                decay = decay_ref[src, lanes] * scale
                push = drive_ref[src, lanes].astype(jnp.float32) * root
                for h in range(2):
                    dst = pl.ds(j * rows + m * 16 * SEGMENTS + h * 8 * SEGMENTS + s, 8, stride=SEGMENTS)
                    rate_ref[dst, :] = decay[h * 8 : h * 8 + 8]
                    push_ref[dst, :] = push[h * 8 : h * 8 + 8]
        return 0

    lax.fori_loop(0, steps // 16, spread, 0)

    def step(i, carry):
        out = []
        for j in range(tiles):
            prod, fwd, bwd = carry[j]
            at = pl.ds(pl.multiple_of(j * rows + i * SEGMENTS, SEGMENTS), SEGMENTS)
            keep = jnp.exp(-rate_ref[at, :])
            push = push_ref[at, :]
            bwd = bwd + prod * push
            fwd = keep * fwd + push
            prod = prod * keep
            out.append((prod, fwd, bwd))
        return tuple(out)

    one = jnp.ones((SEGMENTS, LANES), jnp.float32)
    zero = jnp.zeros((SEGMENTS, LANES), jnp.float32)
    carry = lax.fori_loop(0, steps, step, ((one, zero, zero),) * tiles, unroll=8)
    for j in range(tiles):
        lanes = pl.ds(j * LANES, LANES)
        prod, fwd, bwd = carry[j]
        prod_ref[:, lanes] = prod
        first_ref[:, lanes] = fwd
        last_ref[:, lanes] = bwd
        p, f, b = prod[0:1], fwd[0:1], bwd[0:1]
        for s in range(1, SEGMENTS):
            b = b + p * bwd[s : s + 1]
            f = prod[s : s + 1] * f + fwd[s : s + 1]
            p = p * prod[s : s + 1]
        for n in range(own_ref.shape[0]):
            own_ref[n, 0:1, lanes] = p
            own_ref[n, 1:2, lanes] = jnp.where(n > mine_ref[0], f, b)


def states_kernel(mine_ref, all_ref, prod_ref, first_ref, last_ref, rate_ref, push_ref, gate_ref, gated_ref, power_ref, ent_ref, acc_ref, state_ref):
    rows, width = gate_ref.shape
    steps = rows // SEGMENTS
    tiles = width // LANES
    count = all_ref.shape[0]
    mine = mine_ref[0]
    fwd = jnp.zeros((1, width), jnp.float32)
    bwd = jnp.zeros((1, width), jnp.float32)
    for n in range(count):
        fwd = jnp.where(n < mine, all_ref[n, 0:1, :] * fwd + all_ref[n, 1:2, :], fwd)
    for n in range(count - 1, -1, -1):
        bwd = jnp.where(n > mine, all_ref[n, 0:1, :] * bwd + all_ref[n, 1:2, :], bwd)
    for s in range(SEGMENTS):
        ent_ref[0, s : s + 1, :] = fwd
        fwd = prod_ref[s : s + 1, :] * fwd + first_ref[s : s + 1, :]
    for s in range(SEGMENTS - 1, -1, -1):
        bwd = prod_ref[s : s + 1, :] * bwd + last_ref[s : s + 1, :]
        ent_ref[1, s : s + 1, :] = bwd

    group = 4 if tiles % 4 == 0 else 1
    for g in range(0, tiles, group):

        def step(i, carry):
            out = []
            for j in range(group):
                f, b = carry[j]
                at = pl.ds(pl.multiple_of((g + j) * rows + i * SEGMENTS, SEGMENTS), SEGMENTS)
                x = rate_ref[at, :]
                push = push_ref[at, :]
                f = jnp.exp(-x) * f + push
                state_ref[at, :] = f + b
                b = (b - push) * jnp.exp(x)
                out.append((f, b))
            return tuple(out)

        start = tuple(
            (ent_ref[0, :, pl.ds((g + j) * LANES, LANES)], ent_ref[1, :, pl.ds((g + j) * LANES, LANES)])
            for j in range(group)
        )
        lax.fori_loop(0, steps, step, start, unroll=8)

    def gating(m, _):
        for s in range(SEGMENTS):
            at = pl.ds(pl.multiple_of(s * steps + m * 16, 16), 16)
            acc = jnp.zeros((16, LANES), jnp.float32)
            for j in range(tiles):
                lanes = pl.ds(j * LANES, LANES)
                base = j * rows + m * 16 * SEGMENTS + s
                half = [state_ref[pl.ds(base + h * 8 * SEGMENTS, 8, stride=SEGMENTS), :] for h in range(2)]
                g = jnp.concatenate(half, axis=0) / (1.0 + jnp.exp(-gate_ref[at, lanes].astype(jnp.float32)))
                gated_ref[at, lanes] = g
                acc = acc + g * g
            acc_ref[at, :] = acc
        return 0

    lax.fori_loop(0, steps // 16, gating, 0)
    for r in range(rows // LANES):
        block = acc_ref[r * LANES : (r + 1) * LANES, :].T
        power = jnp.sum(block, axis=0, keepdims=True)
        power_ref[r : r + 1, :] = power


def norm_kernel(channels, *refs):
    *power_refs, gain_ref, gated_ref, out_ref = refs
    rows, width = gated_ref.shape
    for r in range(rows // LANES):
        total = power_refs[0][r : r + 1, :]
        for power_ref in power_refs[1:]:
            total = total + power_ref[r : r + 1, :]
        factor = lax.rsqrt(total / channels + 1e-06)
        factor = jnp.broadcast_to(factor, (LANES, LANES)).T
        at = slice(r * LANES, (r + 1) * LANES)
        for j in range(width // LANES):
            lanes = slice(j * LANES, (j + 1) * LANES)
            out_ref[at, lanes] = (gated_ref[at, lanes] * factor * gain_ref[:, lanes]).astype(jnp.bfloat16)


def held(value):
    return pltpu.with_memory_space_constraint(value, pltpu.VMEM)


def shifts(value, axis):
    count = lax.axis_size(axis)
    return [
        held(lax.ppermute(value, axis, [(n, (n + k) % count) for n in range(count)]))
        for k in range(1, count)
    ]


def body(decay_rate, drive_in, gate_in, norm_gain):
    batch, rows, width = decay_rate.shape
    length = rows * lax.axis_size("sp")
    channels = width * lax.axis_size("tp")
    f32 = jnp.float32
    decay = decay_rate.reshape(rows, width)
    drive = drive_in.reshape(rows, width)
    gate = gate_in.reshape(rows, width)
    block = min(width, 256)
    vmem = pl.BlockSpec(memory_space=pltpu.VMEM)
    cols = lambda r: pl.BlockSpec((r, block), lambda c: (0, c))
    stack = pl.BlockSpec((rows * block // LANES, LANES), lambda c: (c, 0))
    mine = lax.axis_index("sp").astype(jnp.int32).reshape(1)
    own, prod, first, last, rate, push = pl.pallas_call(
        functools.partial(totals_kernel, 1.0 / length, length ** (-0.5)),
        grid=(width // block,),
        in_specs=[pl.BlockSpec(memory_space=pltpu.SMEM), cols(rows), cols(rows)],
        out_specs=[pl.BlockSpec((lax.axis_size("sp"), 2, block), lambda c: (0, 0, c)), cols(SEGMENTS), cols(SEGMENTS), cols(SEGMENTS), stack, stack],
        out_shape=[pltpu.VMEM((lax.axis_size("sp"), 2, width), f32)]
        + [pltpu.VMEM((SEGMENTS, width), f32)] * 3
        + [jax.ShapeDtypeStruct((rows * width // LANES, LANES), f32)] * 2,
        name="totals",
    )(mine, decay, drive)
    others = held(lax.all_to_all(own, "sp", 0, 0, tiled=True))
    gated, power = pl.pallas_call(
        states_kernel,
        in_specs=[pl.BlockSpec(memory_space=pltpu.SMEM)] + [vmem] * 7,
        out_specs=[vmem, vmem],
        out_shape=[jax.ShapeDtypeStruct((rows, width), f32), pltpu.VMEM((rows // LANES, LANES), f32)],
        scratch_shapes=[pltpu.VMEM((2, SEGMENTS, width), f32), pltpu.VMEM((rows, LANES), f32), pltpu.VMEM((rows * width // LANES, LANES), f32)],
        name="states",
    )(mine, others, held(prod), held(first), held(last), rate, push, gate)
    powers = [held(power)] + shifts(power, "tp")
    filtered = pl.pallas_call(
        functools.partial(norm_kernel, float(channels)),
        in_specs=[vmem] * (len(powers) + 2),
        out_specs=vmem,
        out_shape=jax.ShapeDtypeStruct((rows, width), jnp.bfloat16),
        name="norm",
    )(*powers, norm_gain.reshape(1, width), gated)
    return filtered.reshape(batch, rows, width)


def solution(mesh):
    in_specs = (P(None, "sp", "tp"), P(None, "sp", "tp"), P(None, "sp", "tp"), P("tp"))
    out_specs = P(None, "sp", "tp")
    return jax.shard_map(body, mesh=mesh, in_specs=in_specs, out_specs=out_specs, check_vma=False)
```
